32 devices in a mesh: cfg: 2 (over core), tm: 16 (over z, y, x).
Axes of the slice: x: 2, y: 2, z: 4, core: 2. Of those that a mesh axis runs over, the one named last changes fastest.
Arguments:
- queries: bfloat16 [2, 12288, 1152], P('cfg', 'tm'), may hold values from -6 to 6
- key_vectors: bfloat16 [2, 12288, 1152], P('cfg', 'tm'), may hold values from -12 to 12
- value_vectors: bfloat16 [2, 12288, 1152], P('cfg', 'tm'), may hold values from -4 to 4
- out_weight: bfloat16 [1152, 2240], replicated, may hold values from -0.1875 to 0.1875
- first_frame: int32 [32], P('tm'), may hold values from 0 to 31, as said below
Outputs:
- guided: bfloat16 [12288, 2240], P('tm', 'cfg')
The draws below stay inside these ranges and needn't reach their ends.
Inputs may be any that keep to these rules, and one draw needn't show every extreme that they name: first_frame[f] is 0 or lies between f - 4 and f; some frame f has first_frame[f] = f - 4.
All inputs are finite; a program needn't handle non-finite values.
Results may differ from the reference program's by a relative error of at most 0.014.
Values may be sent and summed in bfloat16 or wider, within the bound.
A program may use at most 192 MiB of HBM per device.

```python
import math
import jax
import jax.numpy as jnp
from jax import lax

D = 2240
H = 36
DH = 32
FR = 2
NEAR = 2
FT = 384
HD = 1152
NF = 32
TOKENS = 12288
WIN = 4


def shared_noise(key):
    noise_key = jax.random.fold_in(key, 11)
    return jnp.clip(jax.random.normal(noise_key, (2, NF, FT, H, DH), jnp.float32), -4.0, 4.0)


def draw_key_vectors(key, part):
    noise = shared_noise(key)
    scale_key = jax.random.fold_in(key, 13)
    lowest = 0.3
    scales = jnp.exp(jax.random.uniform(scale_key, (2, NF, 1, H, DH), jnp.float32, math.log(lowest), math.log(3.0)))
    return (noise * scales).reshape(2, NF * FT, H * DH).astype(jnp.bfloat16)


def draw_value_vectors(key, part):
    noise = shared_noise(key)
    mixing_key = jax.random.fold_in(key, 29)
    own_key = jax.random.fold_in(key, 23)
    offset_key = jax.random.fold_in(key, 27)
    mixing = jax.random.normal(mixing_key, (H, DH, DH), jnp.float32) / math.sqrt(DH)
    mixed = jnp.einsum('bgthd,hde->bgthe', noise, mixing)
    coupled = 0.9 * jnp.clip(mixed, -2.5, 2.5)
    own = 0.3 * jnp.clip(jax.random.normal(own_key, (2, NF, FT, H, DH), jnp.float32), -3.0, 3.0)
    offsets = jax.random.uniform(offset_key, (2, NF, 1, H, DH), jnp.float32, -0.8, 0.8)
    return (coupled + own + offsets).reshape(2, NF * FT, H * DH).astype(jnp.bfloat16)


def draw_first_frame(key, part):
    first_key = jax.random.fold_in(key, 31)
    second_key = jax.random.fold_in(key, 37)
    third_key = jax.random.fold_in(key, 41)
    frame_ids = jnp.arange(NF, dtype=jnp.int32)
    windowed = jax.random.randint(first_key, (NF,), 0, 2, dtype=jnp.int32)
    backward = jax.random.randint(second_key, (NF,), 0, WIN + 1, dtype=jnp.int32)
    starts = jnp.where(windowed == 1, jnp.maximum(frame_ids - backward, 0), 0)
    reaching = (frame_ids % FR == 0) & (frame_ids >= FR) & (frame_ids <= NEAR * FR)
    starts = jnp.where(reaching, 1, starts)
    chosen = jax.random.randint(third_key, (), WIN + 1, NF, dtype=jnp.int32)
    starts = jnp.where(frame_ids == chosen, frame_ids - WIN, starts)
    return starts.astype(jnp.int32)


def shard_levels(rng, dims, shards, low, high):
    factor_of = 1.0
    for dim, shards_of in shards:
        draws = jax.random.uniform(jax.random.fold_in(jax.random.fold_in(rng, 6), dim), (shards_of,), jnp.float32, low / len(shards), high / len(shards))
        factor_of = factor_of * jnp.repeat(jnp.exp(draws), dims[dim] // shards_of).reshape((-1,) + (1,) * (len(dims) - 1 - dim))
    return factor_of


def gaussian(stream_key, dims, spread, limit, split=(), held_as=jnp.bfloat16):
    array = spread * jax.random.normal(stream_key, dims, jnp.float32)
    if split:
        array = array * shard_levels(stream_key, dims, split, -0.22, 0.18)
    return jnp.clip(array, -limit, limit).astype(held_as)


def setup_inputs(seed: int = 0) -> dict:
    keys = jax.random.split(jax.random.key(seed), 6)
    return {
        "queries": gaussian(keys[0], (2, TOKENS, HD), 1.0, 6.0, ((0, 2), (1, 16))),
        "key_vectors": draw_key_vectors(jax.random.fold_in(keys[5], 71), 0),
        "value_vectors": draw_value_vectors(jax.random.fold_in(keys[5], 71), 0),
        "out_weight": gaussian(keys[3], (HD, D), HD ** -0.5, 0.1875),
        "first_frame": draw_first_frame(jax.random.fold_in(keys[5], 71), 0),
    }


guide_scale = 4.5
epsilon = 1e-6


def reference(queries, key_vectors, value_vectors, out_weight, first_frame):
    frame_ids = jnp.arange(NF, dtype=jnp.int32)
    starts = first_frame.astype(jnp.int32)
    results = []
    for branch in range(2):
        query_feats = jnp.maximum(queries[branch], 0).astype(jnp.float32).reshape(NF, FT, H, DH)
        key_feats = jnp.maximum(key_vectors[branch], 0).astype(jnp.float32).reshape(NF, FT, H, DH)
        value_feats = value_vectors[branch].astype(jnp.float32).reshape(NF, FT, H, DH)
        frame_states = jnp.einsum("gthd,gthe->ghde", key_feats, value_feats, precision=lax.Precision.HIGHEST)
        frame_sums = jnp.sum(key_feats, axis=1)
        cumulative_states = jnp.concatenate([jnp.zeros((1, H, DH, DH), jnp.float32), jnp.cumsum(frame_states, axis=0)], axis=0)
        cumulative_sums = jnp.concatenate([jnp.zeros((1, H, DH), jnp.float32), jnp.cumsum(frame_sums, axis=0)], axis=0)
        attended_states = cumulative_states[frame_ids + 1] - cumulative_states[starts]
        attended_sums = cumulative_sums[frame_ids + 1] - cumulative_sums[starts]
        numerator = jnp.einsum("gthd,ghde->gthe", query_feats, attended_states, precision=lax.Precision.HIGHEST)
        denominator = jnp.einsum("gthd,ghd->gth", query_feats, attended_sums, precision=lax.Precision.HIGHEST) + epsilon
        attended = (numerator / denominator[..., None]).astype(jnp.bfloat16).reshape(TOKENS, H * DH)
        results.append(jnp.dot(attended, out_weight, preferred_element_type=jnp.float32))
    return (results[1] + guide_scale * (results[0] - results[1])).astype(jnp.bfloat16)
```

```python
import functools

import jax
import jax.numpy as jnp
from jax import lax
from jax.experimental import pallas as pl
from jax.experimental.pallas import tpu as pltpu
from jax.sharding import PartitionSpec as P

DH = 32
NEAR = 2
LANES = 128
PER = LANES // DH

guide_scale = 4.5
epsilon = 1e-06


def head_mask(rows, block):
    row = lax.broadcasted_iota(jnp.int32, (rows, LANES), 0) // DH
    lane = lax.broadcasted_iota(jnp.int32, (rows, LANES), 1) // DH
    return lane == (block if rows == DH else row)


def states_kernel(
    n, bits, ff_ref, q_ref, k_ref, v_ref, st_ref, qo_ref,
    kbuf, vbuf, frames, near_out, near_in, tot, pre, tot_out, tot_in, fin, other,
    load_sem, tot_send, tot_recv, near_send, near_recv, q_sem, fin_sem,
):
    fr = frames.shape[0]
    ft = kbuf.shape[0] // fr
    groups = kbuf.shape[1] // LANES
    base = groups * DH
    me = lax.axis_index("tm")
    other_core = 1 - lax.axis_index("cfg")

    loads = []
    for f in range(fr):
        rows = pl.ds(f * ft, ft)
        for which, (src, dst) in enumerate(((k_ref, kbuf), (v_ref, vbuf))):
            copy = pltpu.make_async_copy(src.at[rows], dst.at[rows], load_sem.at[2 * f + which])
            copy.start()
            loads.append(copy)

    def partner(k):
        bit = (me // (1 << k)) % 2
        return bit, me + (1 - 2 * bit) * (1 << k)

    barrier = pltpu.get_barrier_semaphore()
    pl.semaphore_signal(barrier, inc=1, device_id={"cfg": other_core})
    count = jnp.int32(1 + bits)
    for k in range(bits):
        pl.semaphore_signal(barrier, inc=1, device_id={"tm": partner(k)[1]})
    for d in range(1, NEAR + 1):
        @pl.when(me + d < n)
        def _():
            pl.semaphore_signal(barrier, inc=1, device_id={"tm": me + d})

        @pl.when(me >= d)
        def _():
            pl.semaphore_signal(barrier, inc=1, device_id={"tm": me - d})

        count = count + jnp.where(me + d < n, 1, 0) + jnp.where(me >= d, 1, 0)

    masks = [head_mask(DH, a) for a in range(PER)]
    for f in range(fr):
        loads[2 * f].wait()
        loads[2 * f + 1].wait()
        frames[f, base:, :] = jnp.zeros((frames.shape[1] - base, LANES), jnp.float32)
        for g in range(groups):
            cols = slice(g * LANES, (g + 1) * LANES)
            keys = jnp.maximum(kbuf[f * ft:(f + 1) * ft, cols], 0)
            values = vbuf[f * ft:(f + 1) * ft, cols]
            full = lax.dot_general(
                values, keys, (((0,), (0,)), ((), ())), preferred_element_type=jnp.float32
            )
            compact = jnp.zeros((DH, LANES), jnp.float32)
            for a in range(PER):
                compact = jnp.where(masks[a], full[a * DH:(a + 1) * DH], compact)
            frames[f, g * DH:(g + 1) * DH, :] = compact
            frames[f, base + g:base + g + 1, :] = jnp.sum(
                keys.astype(jnp.float32), axis=0, keepdims=True
            )
    near_out[...] = frames[...].astype(jnp.bfloat16)
    total = frames[0]
    for f in range(1, fr):
        total = total + frames[f]
    tot[...] = total
    tot_out[0] = total.astype(jnp.bfloat16)
    pre[...] = jnp.zeros_like(pre)
    for d in range(1, NEAR + 1):
        @pl.when(me < d)
        def _():
            near_in[d - 1] = jnp.zeros(near_in.shape[1:], jnp.bfloat16)

    pl.semaphore_wait(barrier, count)

    def near_copy(d):
        return pltpu.make_async_remote_copy(
            src_ref=near_out, dst_ref=near_in.at[d - 1], send_sem=near_send.at[d - 1],
            recv_sem=near_recv.at[d - 1], device_id={"tm": me + d},
        )

    def start_near(d):
        @pl.when(me + d < n)
        def _():
            near_copy(d).start()

    q_copy = pltpu.make_async_remote_copy(
        src_ref=q_ref, dst_ref=qo_ref, send_sem=q_sem.at[0], recv_sem=q_sem.at[1],
        device_id={"cfg": other_core},
    )
    for k in range(bits):
        bit, peer = partner(k)
        copy = pltpu.make_async_remote_copy(
            src_ref=tot_out.at[k], dst_ref=tot_in.at[k], send_sem=tot_send.at[k],
            recv_sem=tot_recv.at[k], device_id={"tm": peer},
        )
        if k < bits - 1:
            copy.start()
            if k == 0:
                start_near(2)
                q_copy.start()
            if k == min(1, bits - 2):
                start_near(1)
            copy.wait_recv()
            got = tot_in[k].astype(jnp.float32)
            pre[...] += jnp.where(bit == 1, 1.0, 0.0) * got
            tot[...] += got
            tot_out[k + 1] = tot[...].astype(jnp.bfloat16)
            copy.wait_send()
        else:
            @pl.when(bit == 0)
            def _():
                copy.start()
                copy.wait_send()

            @pl.when(bit == 1)
            def _():
                copy.wait_recv()
                pre[...] += tot_in[k].astype(jnp.float32)

    for d in range(1, NEAR + 1):
        @pl.when(me >= d)
        def _():
            near_copy(d).wait_recv()

        @pl.when(me + d < n)
        def _():
            near_copy(d).wait_send()

    for j in range(fr):
        first = ff_ref[j]
        whole = first == 0
        acc = jnp.where(whole, 1.0, 0.0) * pre[...]
        for f in range(j + 1):
            acc = acc + jnp.where(me * fr + f >= first, 1.0, 0.0) * frames[f]
        for d in range(1, NEAR + 1):
            for f in range(fr):
                inside = jnp.logical_and(first > 0, (me - d) * fr + f >= first)
                acc = acc + jnp.where(inside, 1.0, 0.0) * near_in[d - 1, f].astype(jnp.float32)
        fin[j] = acc
        st_ref[0, j] = acc
    fin_copy = pltpu.make_async_remote_copy(
        src_ref=fin, dst_ref=other, send_sem=fin_sem.at[0], recv_sem=fin_sem.at[1],
        device_id={"cfg": other_core},
    )
    fin_copy.start()
    fin_copy.wait()
    st_ref[1] = other[...]
    q_copy.wait()


def project_kernel(per_frame, st_ref, q_ref, qo_ref, w_ref, o_ref, mats, comb):
    groups = q_ref.shape[1] // LANES
    base = groups * DH
    core = lax.axis_index("cfg")
    own_scale = jnp.where(core == 0, guide_scale, 1.0 - guide_scale)
    other_scale = jnp.where(core == 0, 1.0 - guide_scale, guide_scale)

    @pl.when(pl.program_id(0) % per_frame == 0)
    def _():
        frame = pl.program_id(0) // per_frame
        diagonal = head_mask(LANES, 0)
        for b in range(2):
            for g in range(groups):
                compact = st_ref[b, frame, g * DH:(g + 1) * DH, :]
                sums = st_ref[b, frame, base + g:base + g + 1, :]
                state = jnp.where(diagonal, jnp.concatenate([compact] * PER, axis=0), 0.0)
                total = jnp.where(diagonal, jnp.broadcast_to(sums, (LANES, LANES)), 0.0)
                both = jnp.concatenate([state, total], axis=0)
                upper = both.astype(jnp.bfloat16)
                lower = (both - upper.astype(jnp.float32)).astype(jnp.bfloat16)
                mats[b, g] = jnp.concatenate([upper, lower], axis=1)

    for g in range(groups):
        cols = slice(g * LANES, (g + 1) * LANES)
        parts = []
        for b, ref in enumerate((q_ref, qo_ref)):
            feats = jnp.maximum(ref[:, cols], 0)
            both = lax.dot_general(
                jnp.concatenate([feats, feats], axis=1), mats[b, g],
                (((1,), (1,)), ((), ())), preferred_element_type=jnp.float32,
            )
            parts.append((both[:, :LANES], both[:, LANES:] + epsilon))
        (own, own_den), (oth, oth_den) = parts
        mixed = (own_scale * own * oth_den + other_scale * oth * own_den) / (own_den * oth_den)
        comb[:, cols] = mixed.astype(jnp.bfloat16)
    o_ref[...] = jnp.dot(
        comb[...], w_ref[...], preferred_element_type=jnp.float32
    ).astype(o_ref.dtype)


def on_device(n, cores, queries, key_vectors, value_vectors, out_weight, first_frame):
    rows, width = queries.shape[1:]
    fr = first_frame.shape[0]
    bits = n.bit_length() - 1
    groups = width // LANES
    height = groups * DH + 16 * pl.cdiv(groups, 16)
    block = (height, LANES)
    flat = lambda a: a.reshape(rows, width)
    queries = flat(queries)
    f32, bf16 = jnp.float32, jnp.bfloat16
    hbm = pl.BlockSpec(memory_space=pl.ANY)
    vmem = pl.BlockSpec(memory_space=pltpu.VMEM)
    states, other_queries = pl.pallas_call(
        functools.partial(states_kernel, n, bits),
        name="states",
        out_shape=(
            jax.ShapeDtypeStruct((2, fr) + block, f32),
            jax.ShapeDtypeStruct((rows, width), bf16),
        ),
        in_specs=[pl.BlockSpec(memory_space=pltpu.SMEM), hbm, hbm, hbm],
        out_specs=(vmem, hbm),
        scratch_shapes=[
            pltpu.VMEM((rows, width), bf16),
            pltpu.VMEM((rows, width), bf16),
            pltpu.VMEM((fr,) + block, f32),
            pltpu.VMEM((fr,) + block, bf16),
            pltpu.VMEM((NEAR, fr) + block, bf16),
            pltpu.VMEM(block, f32),
            pltpu.VMEM(block, f32),
            pltpu.VMEM((bits,) + block, bf16),
            pltpu.VMEM((bits,) + block, bf16),
            pltpu.VMEM((fr,) + block, f32),
            pltpu.VMEM((fr,) + block, f32),
            pltpu.SemaphoreType.DMA((2 * fr,)),
            pltpu.SemaphoreType.DMA((bits,)),
            pltpu.SemaphoreType.DMA((bits,)),
            pltpu.SemaphoreType.DMA((NEAR,)),
            pltpu.SemaphoreType.DMA((NEAR,)),
            pltpu.SemaphoreType.DMA((2,)),
            pltpu.SemaphoreType.DMA((2,)),
        ],
        compiler_params=pltpu.CompilerParams(
            collective_id=0, has_side_effects=True, vmem_limit_bytes=24 << 20
        ),
    )(first_frame, queries, flat(key_vectors), flat(value_vectors))

    columns = out_weight.shape[1] // cores
    weight = lax.dynamic_slice_in_dim(
        out_weight, lax.axis_index("cfg") * columns, columns, axis=1
    )
    per_frame = 2
    tile = rows // (fr * per_frame)
    return pl.pallas_call(
        functools.partial(project_kernel, per_frame),
        name="project",
        grid=(fr * per_frame,),
        out_shape=jax.ShapeDtypeStruct((rows, columns), bf16),
        in_specs=[
            pl.BlockSpec((2, fr) + block, lambda i: (0, 0, 0, 0)),
            pl.BlockSpec((tile, width), lambda i: (i, 0)),
            pl.BlockSpec((tile, width), lambda i: (i, 0)),
            pl.BlockSpec((width, columns), lambda i: (0, 0)),
        ],
        out_specs=pl.BlockSpec((tile, columns), lambda i: (i, 0)),
        scratch_shapes=[
            pltpu.VMEM((2, groups, 2 * LANES, 2 * LANES), bf16),
            pltpu.VMEM((tile, width), bf16),
        ],
        compiler_params=pltpu.CompilerParams(
            dimension_semantics=("arbitrary",), vmem_limit_bytes=32 << 20
        ),
    )(states, queries, other_queries, weight)


def solution(mesh):
    placed = (P("cfg", "tm", None), P("cfg", "tm", None), P("cfg", "tm", None), P(), P("tm"))
    return jax.shard_map(
        functools.partial(on_device, mesh.shape["tm"], mesh.shape["cfg"]),
        mesh=mesh, in_specs=placed, out_specs=P("tm", "cfg"), check_vma=False,
    )
```

```python
import functools

import jax
import jax.numpy as jnp
from jax import lax
from jax.experimental import pallas as pl
from jax.experimental.pallas import tpu as pltpu
from jax.sharding import PartitionSpec as P

DH = 32
NEAR = 2
LANES = 128
PER = LANES // DH

guide_scale = 4.5
epsilon = 1e-06


def head_mask(rows, block):
    row = lax.broadcasted_iota(jnp.int32, (rows, LANES), 0) // DH
    lane = lax.broadcasted_iota(jnp.int32, (rows, LANES), 1) // DH
    return lane == (block if rows == DH else row)


def states_kernel(
    n, bits, ff_ref, q_ref, k_ref, v_ref, st_ref, qo_ref,
    kbuf, vbuf, frames, near_out, near_in, tot, pre, tot_out, tot_in, fin, other,
    load_sem, tot_send, tot_recv, near_send, near_recv, q_sem, fin_sem,
):
    fr = frames.shape[0]
    ft = kbuf.shape[0] // fr
    groups = kbuf.shape[1] // LANES
    base = groups * DH
    me = lax.axis_index("tm")
    other_core = 1 - lax.axis_index("cfg")

    loads = []
    for f in range(fr):
        rows = pl.ds(f * ft, ft)
        for which, (src, dst) in enumerate(((k_ref, kbuf), (v_ref, vbuf))):
            copy = pltpu.make_async_copy(src.at[rows], dst.at[rows], load_sem.at[2 * f + which])
            copy.start()
            loads.append(copy)

    def partner(k):
        bit = (me // (1 << k)) % 2
        return bit, me + (1 - 2 * bit) * (1 << k)

    barrier = pltpu.get_barrier_semaphore()
    pl.semaphore_signal(barrier, inc=1, device_id={"cfg": other_core})
    count = jnp.int32(1 + bits)
    for k in range(bits):
        pl.semaphore_signal(barrier, inc=1, device_id={"tm": partner(k)[1]})
    for d in range(1, NEAR + 1):
        @pl.when(me + d < n)
        def _():
            pl.semaphore_signal(barrier, inc=1, device_id={"tm": me + d})

        @pl.when(me >= d)
        def _():
            pl.semaphore_signal(barrier, inc=1, device_id={"tm": me - d})

        count = count + jnp.where(me + d < n, 1, 0) + jnp.where(me >= d, 1, 0)

    masks = [head_mask(DH, a) for a in range(PER)]
    for f in range(fr):
        loads[2 * f].wait()
        loads[2 * f + 1].wait()
        frames[f, base:, :] = jnp.zeros((frames.shape[1] - base, LANES), jnp.float32)
        for g in range(groups):
            cols = slice(g * LANES, (g + 1) * LANES)
            keys = jnp.maximum(kbuf[f * ft:(f + 1) * ft, cols], 0)
            values = vbuf[f * ft:(f + 1) * ft, cols]
            full = lax.dot_general(
                values, keys, (((0,), (0,)), ((), ())), preferred_element_type=jnp.float32
            )
            compact = jnp.zeros((DH, LANES), jnp.float32)
            for a in range(PER):
                compact = jnp.where(masks[a], full[a * DH:(a + 1) * DH], compact)
            frames[f, g * DH:(g + 1) * DH, :] = compact
            frames[f, base + g:base + g + 1, :] = jnp.sum(
                keys.astype(jnp.float32), axis=0, keepdims=True
            )
    near_out[...] = frames[...].astype(jnp.bfloat16)
    total = frames[0]
    for f in range(1, fr):
        total = total + frames[f]
    tot[...] = total
    tot_out[0] = total.astype(jnp.bfloat16)
    pre[...] = jnp.zeros_like(pre)
    for d in range(1, NEAR + 1):
        @pl.when(me < d)
        def _():
            near_in[d - 1] = jnp.zeros(near_in.shape[1:], jnp.bfloat16)

    pl.semaphore_wait(barrier, count)

    def near_copy(d):
        return pltpu.make_async_remote_copy(
            src_ref=near_out, dst_ref=near_in.at[d - 1], send_sem=near_send.at[d - 1],
            recv_sem=near_recv.at[d - 1], device_id={"tm": me + d},
        )

    def start_near(d):
        @pl.when(me + d < n)
        def _():
            near_copy(d).start()

    q_copy = pltpu.make_async_remote_copy(
        src_ref=q_ref, dst_ref=qo_ref, send_sem=q_sem.at[0], recv_sem=q_sem.at[1],
        device_id={"cfg": other_core},
    )
    for k in range(bits):
        bit, peer = partner(k)
        copy = pltpu.make_async_remote_copy(
            src_ref=tot_out.at[k], dst_ref=tot_in.at[k], send_sem=tot_send.at[k],
            recv_sem=tot_recv.at[k], device_id={"tm": peer},
        )
        if k < bits - 1:
            copy.start()
            if k == 0:
                start_near(2)
                q_copy.start()
            if k == min(1, bits - 2):
                start_near(1)
            copy.wait_recv()
            got = tot_in[k].astype(jnp.float32)
            pre[...] += jnp.where(bit == 1, 1.0, 0.0) * got
            tot[...] += got
            tot_out[k + 1] = tot[...].astype(jnp.bfloat16)
            copy.wait_send()
        else:
            @pl.when(bit == 0)
            def _():
                copy.start()
                copy.wait_send()

            @pl.when(bit == 1)
            def _():
                copy.wait_recv()
                pre[...] += tot_in[k].astype(jnp.float32)

    for d in range(1, NEAR + 1):
        @pl.when(me >= d)
        def _():
            near_copy(d).wait_recv()

        @pl.when(me + d < n)
        def _():
            near_copy(d).wait_send()

    for j in range(fr):
        first = ff_ref[j]
        whole = first == 0
        acc = jnp.where(whole, 1.0, 0.0) * pre[...]
        for f in range(j + 1):
            acc = acc + jnp.where(me * fr + f >= first, 1.0, 0.0) * frames[f]
        for d in range(1, NEAR + 1):
            for f in range(fr):
                inside = jnp.logical_and(first > 0, (me - d) * fr + f >= first)
                acc = acc + jnp.where(inside, 1.0, 0.0) * near_in[d - 1, f].astype(jnp.float32)
        fin[j] = acc
        st_ref[0, j] = acc
    fin_copy = pltpu.make_async_remote_copy(
        src_ref=fin, dst_ref=other, send_sem=fin_sem.at[0], recv_sem=fin_sem.at[1],
        device_id={"cfg": other_core},
    )
    fin_copy.start()
    fin_copy.wait()
    st_ref[1] = other[...]
    q_copy.wait()


def project_kernel(st_ref, q_ref, qo_ref, w_ref, o_ref, qbuf, wbuf, comb, obuf, load_sem, out_sem):
    fr = st_ref.shape[1]
    columns = wbuf.shape[0]
    groups = q_ref.shape[1] // LANES
    base = groups * DH
    ft = comb.shape[0] // fr
    tile = ft if ft % 256 == 0 else 2 * LANES
    core = lax.axis_index("cfg")
    q_copies = [
        pltpu.make_async_copy(src, qbuf.at[b], load_sem.at[1 + b])
        for b, src in enumerate((q_ref, qo_ref))
    ]
    for copy in q_copies:
        copy.start()
    w_copy = pltpu.make_async_copy(
        w_ref.at[pl.ds(pl.multiple_of(core * columns, 16), columns)], wbuf, load_sem.at[0]
    )
    w_copy.start()
    own_scale = jnp.where(core == 0, guide_scale, 1.0 - guide_scale)
    other_scale = jnp.where(core == 0, 1.0 - guide_scale, guide_scale)
    diagonal = head_mask(LANES, 0)

    def matrices(b, frame, g):
        compact = st_ref[b, frame, g * DH:(g + 1) * DH, :]
        sums = st_ref[b, frame, base + g:base + g + 1, :]
        state = jnp.where(diagonal, jnp.concatenate([compact] * PER, axis=0), 0.0)
        total = jnp.where(diagonal, jnp.broadcast_to(sums, (LANES, LANES)), 0.0)
        both = jnp.concatenate([state, total], axis=0)
        upper = both.astype(jnp.bfloat16)
        lower = (both - upper.astype(jnp.float32)).astype(jnp.bfloat16)
        return jnp.concatenate([upper, lower], axis=1)

    for copy in q_copies:
        copy.wait()
    for f in range(fr):
        rows = slice(f * ft, (f + 1) * ft)
        for g in range(groups):
            cols = slice(g * LANES, (g + 1) * LANES)
            parts = []
            for b in range(2):
                feats = jnp.maximum(qbuf[b, rows, cols], 0)
                both = lax.dot_general(
                    jnp.concatenate([feats, feats], axis=1), matrices(b, f, g),
                    (((1,), (1,)), ((), ())), preferred_element_type=jnp.float32,
                )
                parts.append((both[:, :LANES], both[:, LANES:] + epsilon))
            (own, own_den), (oth, oth_den) = parts
            mixed = (own_scale * own * oth_den + other_scale * oth * own_den) / (own_den * oth_den)
            comb[rows, cols] = mixed.astype(jnp.bfloat16)
    w_copy.wait()
    outs = []
    for t in range(comb.shape[0] // tile):
        part = slice(t * tile, (t + 1) * tile)
        obuf[:, part] = lax.dot_general(
            wbuf[...], comb[part, :], (((1,), (1,)), ((), ())),
            preferred_element_type=jnp.float32,
        ).astype(obuf.dtype)
        span = pl.ds(t * tile, tile)
        copy = pltpu.make_async_copy(obuf.at[:, span], o_ref.at[:, span], out_sem.at[t])
        copy.start()
        outs.append(copy)
    for copy in outs:
        copy.wait()


def on_device(n, cores, queries, key_vectors, value_vectors, out_weight, first_frame):
    rows, width = queries.shape[1:]
    fr = first_frame.shape[0]
    bits = n.bit_length() - 1
    groups = width // LANES
    height = groups * DH + 16 * pl.cdiv(groups, 16)
    block = (height, LANES)
    flat = lambda a: a.reshape(rows, width)
    queries = flat(queries)
    f32, bf16 = jnp.float32, jnp.bfloat16
    hbm = pl.BlockSpec(memory_space=pltpu.HBM)
    vmem = pl.BlockSpec(memory_space=pltpu.VMEM)
    states, other_queries = pl.pallas_call(
        functools.partial(states_kernel, n, bits),
        name="states",
        out_shape=(
            jax.ShapeDtypeStruct((2, fr) + block, f32),
            jax.ShapeDtypeStruct((rows, width), bf16),
        ),
        in_specs=[pl.BlockSpec(memory_space=pltpu.SMEM), hbm, hbm, hbm],
        out_specs=(vmem, hbm),
        scratch_shapes=[
            pltpu.VMEM((rows, width), bf16),
            pltpu.VMEM((rows, width), bf16),
            pltpu.VMEM((fr,) + block, f32),
            pltpu.VMEM((fr,) + block, bf16),
            pltpu.VMEM((NEAR, fr) + block, bf16),
            pltpu.VMEM(block, f32),
            pltpu.VMEM(block, f32),
            pltpu.VMEM((bits,) + block, bf16),
            pltpu.VMEM((bits,) + block, bf16),
            pltpu.VMEM((fr,) + block, f32),
            pltpu.VMEM((fr,) + block, f32),
            pltpu.SemaphoreType.DMA((2 * fr,)),
            pltpu.SemaphoreType.DMA((bits,)),
            pltpu.SemaphoreType.DMA((bits,)),
            pltpu.SemaphoreType.DMA((NEAR,)),
            pltpu.SemaphoreType.DMA((NEAR,)),
            pltpu.SemaphoreType.DMA((2,)),
            pltpu.SemaphoreType.DMA((2,)),
        ],
        compiler_params=pltpu.CompilerParams(
            collective_id=0, has_side_effects=True
        ),
    )(first_frame, queries, flat(key_vectors), flat(value_vectors))

    columns = out_weight.shape[1] // cores
    flipped = pl.pallas_call(
        project_kernel,
        name="project",
        out_shape=jax.ShapeDtypeStruct((columns, rows), bf16),
        in_specs=[vmem, hbm, hbm, hbm],
        out_specs=hbm,
        scratch_shapes=[
            pltpu.VMEM((2, rows, width), bf16),
            pltpu.VMEM((columns, width), bf16),
            pltpu.VMEM((rows, width), bf16),
            pltpu.VMEM((columns, rows), bf16),
            pltpu.SemaphoreType.DMA((3,)),
            pltpu.SemaphoreType.DMA((rows // LANES,)),
        ],
            )(states, queries, other_queries, out_weight.T)
    return flipped.T


def solution(mesh):
    placed = (P("cfg", "tm", None), P("cfg", "tm", None), P("cfg", "tm", None), P(), P("tm"))
    return jax.shard_map(
        functools.partial(on_device, mesh.shape["tm"], mesh.shape["cfg"]),
        mesh=mesh, in_specs=placed, out_specs=P("tm", "cfg"), check_vma=False,
    )
```

```python
import functools

import jax
import jax.numpy as jnp
from jax import lax
from jax.experimental import pallas as pl
from jax.experimental.pallas import tpu as pltpu
from jax.sharding import PartitionSpec as P

DH = 32
NEAR = 2
LANES = 128
PER = LANES // DH
CHUNKS = 3

guide_scale = 4.5
epsilon = 1e-06


def head_mask(rows, block):
    row = lax.broadcasted_iota(jnp.int32, (rows, LANES), 0) // DH
    lane = lax.broadcasted_iota(jnp.int32, (rows, LANES), 1) // DH
    return lane == (block if rows == DH else row)


def split_rows(height):
    units = height // 16
    sizes = [(units * (c + 1)) // CHUNKS - (units * c) // CHUNKS for c in range(CHUNKS)]
    return [(16 * sum(sizes[:c]), 16 * sizes[c]) for c in range(CHUNKS)]


def guided_kernel(
    n, bits, ff_ref, q_ref, k_ref, v_ref, w_ref, o_ref,
    kbuf, vbuf, qbuf, wbuf, own_att, comb, obuf, frames, near_out, near_in, tot, pre, tot_out, tot_in, fin, other,
    load_sem, late_sem, out_sem, tot_send, tot_recv, near_send, near_recv, q_sem, fin_sem,
):
    fr = frames.shape[0]
    ft = kbuf.shape[0] // fr
    groups = kbuf.shape[1] // LANES
    base = groups * DH
    chunks = split_rows(frames.shape[1])
    me = lax.axis_index("tm")
    other_core = 1 - lax.axis_index("cfg")

    loads = []
    for f in range(fr):
        rows = pl.ds(f * ft, ft)
        for which, (src, dst) in enumerate(((k_ref, kbuf), (v_ref, vbuf))):
            copy = pltpu.make_async_copy(src.at[rows], dst.at[rows], load_sem.at[2 * f + which])
            copy.start()
            loads.append(copy)

    def partner(k):
        bit = (me // (1 << k)) % 2
        return bit, me + (1 - 2 * bit) * (1 << k)

    barrier = pltpu.get_barrier_semaphore()
    pl.semaphore_signal(barrier, inc=1, device_id={"cfg": other_core})
    count = jnp.int32(1 + bits)
    for k in range(bits):
        pl.semaphore_signal(barrier, inc=1, device_id={"tm": partner(k)[1]})
    for d in range(1, NEAR + 1):
        @pl.when(me + d < n)
        def _():
            pl.semaphore_signal(barrier, inc=1, device_id={"tm": me + d})

        @pl.when(me >= d)
        def _():
            pl.semaphore_signal(barrier, inc=1, device_id={"tm": me - d})

        count = count + jnp.where(me + d < n, 1, 0) + jnp.where(me >= d, 1, 0)

    masks = [head_mask(DH, a) for a in range(PER)]
    for f in range(fr):
        loads[2 * f].wait()
        loads[2 * f + 1].wait()
        frames[f, base:, :] = jnp.zeros((frames.shape[1] - base, LANES), jnp.float32)
        for g in range(groups):
            cols = slice(g * LANES, (g + 1) * LANES)
            keys = jnp.maximum(kbuf[f * ft:(f + 1) * ft, cols], 0)
            values = vbuf[f * ft:(f + 1) * ft, cols]
            full = lax.dot_general(
                values, keys, (((0,), (0,)), ((), ())), preferred_element_type=jnp.float32
            )
            compact = jnp.zeros((DH, LANES), jnp.float32)
            for a in range(PER):
                compact = jnp.where(masks[a], full[a * DH:(a + 1) * DH], compact)
            frames[f, g * DH:(g + 1) * DH, :] = compact
            frames[f, base + g:base + g + 1, :] = jnp.sum(
                keys.astype(jnp.float32), axis=0, keepdims=True
            )
    columns = wbuf.shape[0]
    late = [
        pltpu.make_async_copy(q_ref, qbuf.at[0], late_sem.at[0]),
        pltpu.make_async_copy(
            w_ref.at[pl.ds(pl.multiple_of((1 - other_core) * columns, 16), columns)],
            wbuf, late_sem.at[1],
        ),
    ]
    for copy in late:
        copy.start()
    near_out[...] = frames[...].astype(jnp.bfloat16)
    total = frames[0]
    for f in range(1, fr):
        total = total + frames[f]
    tot[...] = total
    tot_out[0] = total.astype(jnp.bfloat16)
    pre[...] = jnp.zeros_like(pre)
    for d in range(1, NEAR + 1):
        @pl.when(me < d)
        def _():
            near_in[d - 1] = jnp.zeros(near_in.shape[1:], jnp.bfloat16)

    pl.semaphore_wait(barrier, count)

    def near_copy(d):
        return pltpu.make_async_remote_copy(
            src_ref=near_out, dst_ref=near_in.at[d - 1], send_sem=near_send.at[d - 1],
            recv_sem=near_recv.at[d - 1], device_id={"tm": me + d},
        )

    def start_near(d):
        @pl.when(me + d < n)
        def _():
            near_copy(d).start()

    q_copy = pltpu.make_async_remote_copy(
        src_ref=q_ref, dst_ref=qbuf.at[1], send_sem=q_sem.at[0], recv_sem=q_sem.at[1],
        device_id={"cfg": other_core},
    )
    def total_copy(k, c):
        part = pl.ds(*chunks[c])
        return pltpu.make_async_remote_copy(
            src_ref=tot_out.at[k, part], dst_ref=tot_in.at[k, part],
            send_sem=tot_send.at[k, c], recv_sem=tot_recv.at[k, c],
            device_id={"tm": partner(k)[1]},
        )

    def send_total(k, c):
        if k < bits - 1:
            total_copy(k, c).start()
        else:
            @pl.when(partner(k)[0] == 0)
            def _():
                total_copy(k, c).start()

    for c in range(len(chunks)):
        send_total(0, c)
    start_near(2)
    q_copy.start()
    for k in range(bits):
        bit = partner(k)[0]
        for c, (lo, size) in enumerate(chunks):
            part = slice(lo, lo + size)
            if k < bits - 1:
                total_copy(k, c).wait_recv()
                got = tot_in[k, part].astype(jnp.float32)
                pre[part] += jnp.where(bit == 1, 1.0, 0.0) * got
                summed = tot[part] + got
                tot[part] = summed
                tot_out[k + 1, part] = summed.astype(jnp.bfloat16)
                send_total(k + 1, c)
            else:
                @pl.when(bit == 1)
                def _():
                    total_copy(k, c).wait_recv()
                    pre[part] += tot_in[k, part].astype(jnp.float32)
        if k == 0:
            start_near(1)
    for k in range(bits):
        for c in range(len(chunks)):
            if k < bits - 1:
                total_copy(k, c).wait_send()
            else:
                @pl.when(partner(k)[0] == 0)
                def _():
                    total_copy(k, c).wait_send()

    for d in range(1, NEAR + 1):
        @pl.when(me >= d)
        def _():
            near_copy(d).wait_recv()

        @pl.when(me + d < n)
        def _():
            near_copy(d).wait_send()

    for j in range(fr):
        first = ff_ref[j]
        whole = first == 0
        acc = jnp.where(whole, 1.0, 0.0) * pre[...]
        for f in range(j + 1):
            acc = acc + jnp.where(me * fr + f >= first, 1.0, 0.0) * frames[f]
        for d in range(1, NEAR + 1):
            for f in range(fr):
                inside = jnp.logical_and(first > 0, (me - d) * fr + f >= first)
                acc = acc + jnp.where(inside, 1.0, 0.0) * near_in[d - 1, f].astype(jnp.float32)
        fin[j] = acc
    fin_copy = pltpu.make_async_remote_copy(
        src_ref=fin, dst_ref=other, send_sem=fin_sem.at[0], recv_sem=fin_sem.at[1],
        device_id={"cfg": other_core},
    )
    fin_copy.start()

    own_scale = jnp.where(other_core == 1, guide_scale, 1.0 - guide_scale)
    other_scale = 1.0 - own_scale
    diagonal = head_mask(LANES, 0)
    tile = ft if ft % 256 == 0 else 2 * LANES

    def attended(b, source, f, g):
        rows = slice(f * ft, (f + 1) * ft)
        cols = slice(g * LANES, (g + 1) * LANES)
        compact = source[f, g * DH:(g + 1) * DH, :]
        sums = source[f, base + g:base + g + 1, :]
        state = jnp.where(diagonal, jnp.concatenate([compact] * PER, axis=0), 0.0)
        total = jnp.where(diagonal, jnp.broadcast_to(sums, (LANES, LANES)), 0.0)
        both = jnp.concatenate([state, total], axis=0)
        upper = both.astype(jnp.bfloat16)
        lower = (both - upper.astype(jnp.float32)).astype(jnp.bfloat16)
        feats = jnp.maximum(qbuf[b, rows, cols], 0)
        both = lax.dot_general(
            jnp.concatenate([feats, feats], axis=1),
            jnp.concatenate([upper, lower], axis=1),
            (((1,), (1,)), ((), ())), preferred_element_type=jnp.float32,
        )
        return rows, cols, both[:, :LANES] / (both[:, LANES:] + epsilon)

    late[0].wait()
    for f in range(fr):
        for g in range(groups):
            rows, cols, value = attended(0, fin, f, g)
            own_att[rows, cols] = own_scale * value
    fin_copy.wait()
    q_copy.wait()
    for f in range(fr):
        for g in range(groups):
            rows, cols, value = attended(1, other, f, g)
            comb[rows, cols] = (own_att[rows, cols] + other_scale * value).astype(jnp.bfloat16)
    late[1].wait()
    outs = []
    for t in range(comb.shape[0] // tile):
        part = slice(t * tile, (t + 1) * tile)
        obuf[:, part] = lax.dot_general(
            wbuf[...], comb[part, :], (((1,), (1,)), ((), ())),
            preferred_element_type=jnp.float32,
        ).astype(obuf.dtype)
        span = pl.ds(t * tile, tile)
        copy = pltpu.make_async_copy(obuf.at[:, span], o_ref.at[:, span], out_sem.at[t])
        copy.start()
        outs.append(copy)
    for copy in outs:
        copy.wait()


def on_device(n, cores, queries, key_vectors, value_vectors, out_weight, first_frame):
    rows, width = queries.shape[1:]
    fr = first_frame.shape[0]
    bits = n.bit_length() - 1
    groups = width // LANES
    height = groups * DH + 16 * pl.cdiv(groups, 16)
    block = (height, LANES)
    flat = lambda a: a.reshape(rows, width)
    queries = flat(queries)
    f32, bf16 = jnp.float32, jnp.bfloat16
    hbm = pl.BlockSpec(memory_space=pltpu.HBM)
    columns = out_weight.shape[1] // cores
    flipped = pl.pallas_call(
        functools.partial(guided_kernel, n, bits),
        name="guided",
        out_shape=jax.ShapeDtypeStruct((columns, rows), bf16),
        in_specs=[pl.BlockSpec(memory_space=pltpu.SMEM), hbm, hbm, hbm, hbm],
        out_specs=hbm,
        scratch_shapes=[
            pltpu.VMEM((rows, width), bf16),
            pltpu.VMEM((rows, width), bf16),
            pltpu.VMEM((2, rows, width), bf16),
            pltpu.VMEM((columns, width), bf16),
            pltpu.VMEM((rows, width), f32),
            pltpu.VMEM((rows, width), bf16),
            pltpu.VMEM((columns, rows), bf16),
            pltpu.VMEM((fr,) + block, f32),
            pltpu.VMEM((fr,) + block, bf16),
            pltpu.VMEM((NEAR, fr) + block, bf16),
            pltpu.VMEM(block, f32),
            pltpu.VMEM(block, f32),
            pltpu.VMEM((bits,) + block, bf16),
            pltpu.VMEM((bits,) + block, bf16),
            pltpu.VMEM((fr,) + block, f32),
            pltpu.VMEM((fr,) + block, f32),
            pltpu.SemaphoreType.DMA((2 * fr,)),
            pltpu.SemaphoreType.DMA((2,)),
            pltpu.SemaphoreType.DMA((rows // LANES,)),
            pltpu.SemaphoreType.DMA((bits, CHUNKS)),
            pltpu.SemaphoreType.DMA((bits, CHUNKS)),
            pltpu.SemaphoreType.DMA((NEAR,)),
            pltpu.SemaphoreType.DMA((NEAR,)),
            pltpu.SemaphoreType.DMA((2,)),
            pltpu.SemaphoreType.DMA((2,)),
        ],
        compiler_params=pltpu.CompilerParams(
            collective_id=0, has_side_effects=True
        ),
    )(first_frame, queries, flat(key_vectors), flat(value_vectors), out_weight.T)

    return flipped.T


def solution(mesh):
    placed = (P("cfg", "tm", None), P("cfg", "tm", None), P("cfg", "tm", None), P(), P("tm"))
    return jax.shard_map(
        functools.partial(on_device, mesh.shape["tm"], mesh.shape["cfg"]),
        mesh=mesh, in_specs=placed, out_specs=P("tm", "cfg"), check_vma=False,
    )
```
